32 devices in a mesh: gx: 2 (over x), gy: 4 (over y, core), gz: 4 (over z).
Axes of the slice: x: 2, y: 2, z: 4, core: 2. Of those that a mesh axis runs over, the one named last changes fastest.
Arguments:
- inputs: bfloat16 [640, 8192], P(('gx', 'gz'), 'gy'), may hold values from -6 to 6
- out_grad: bfloat16 [640, 8192], P(('gx', 'gz'), 'gy'), may hold values from -6 to 6
- gate_weight: bfloat16 [8192, 16384], P('gy', ('gx', 'gz')), may hold values from -0.0625 to 0.0625
- up_weight: bfloat16 [8192, 16384], P('gy', ('gx', 'gz')), may hold values from -0.0625 to 0.0625
- down_weight: bfloat16 [16384, 8192], P(('gx', 'gz'), 'gy'), may hold values from -0.046875 to 0.046875
Outputs:
- in_grad: bfloat16 [640, 8192], P(('gx', 'gz'), 'gy')
The draws below stay inside these ranges and needn't reach their ends.
All inputs are finite; a program needn't handle non-finite values.
Results may differ from the reference program's by a relative error of at most 0.0049.
Values may be sent and summed in bfloat16 or wider, within the bound.
A program may use at most 128 MiB of HBM per device.

```python
import jax
import jax.numpy as jnp
from jax import lax

D = 8192
FF = 16384
TOKENS = 640


def shard_levels(rng, shape, split, least, top_value):
    gain = 1.0
    for dim, shards_of in split:
        heights = jax.random.uniform(jax.random.fold_in(jax.random.fold_in(rng, 6), dim), (shards_of,), jnp.float32, least / len(split), top_value / len(split))
        gain = gain * jnp.repeat(jnp.exp(heights), shape[dim] // shards_of).reshape((-1,) + (1,) * (len(shape) - 1 - dim))
    return gain


def bell_draw(key, shape, deviation, bound, pieces=(), held_as=jnp.bfloat16):
    factor_of = shard_levels(key, shape, pieces, -0.22, 0.18) if pieces else 1.0
    result = jax.random.normal(key, shape, jnp.float32) * deviation * factor_of
    return jnp.minimum(jnp.maximum(result, -bound), bound).astype(held_as)


def setup_inputs(seed: int = 0) -> dict:
    arg_keys = jax.random.split(jax.random.key(seed), 6)
    return {
        "inputs": bell_draw(arg_keys[0], (TOKENS, D), 1.0, 6.0, ((0, 8), (1, 4))),
        "out_grad": bell_draw(arg_keys[1], (TOKENS, D), 1.0, 6.0, ((0, 8), (1, 4))),
        "gate_weight": bell_draw(arg_keys[2], (D, FF), D ** -0.5, 0.0625, ((0, 4), (1, 8))),
        "up_weight": bell_draw(arg_keys[3], (D, FF), D ** -0.5, 0.0625, ((0, 4), (1, 8))),
        "down_weight": bell_draw(arg_keys[4], (FF, D), FF ** -0.5, 0.046875, ((0, 8), (1, 4))),
    }


def contract_last(left, right):
    return lax.dot_general(left, right, (((1,), (1,)), ((), ())), preferred_element_type=jnp.float32)


def reference(inputs, out_grad, gate_weight, up_weight, down_weight):
    gate = jnp.dot(inputs, gate_weight, preferred_element_type=jnp.float32)
    upper = jnp.dot(inputs, up_weight, preferred_element_type=jnp.float32)
    hidden_grad = contract_last(out_grad, down_weight)
    logistic = jax.nn.sigmoid(gate)
    gate_grad = (hidden_grad * upper * logistic * (1.0 + gate * (1.0 - logistic))).astype(jnp.bfloat16)
    up_grad = (hidden_grad * gate * logistic).astype(jnp.bfloat16)
    total = contract_last(gate_grad, gate_weight) + contract_last(up_grad, up_weight)
    return total.astype(jnp.bfloat16)
```

```python
import jax
import jax.numpy as jnp
from jax import lax
from jax.sharding import PartitionSpec as P


F32, BF16 = jnp.float32, jnp.bfloat16


def swap(value, axis, size, offset):
    if offset == 0:
        return value
    return lax.ppermute(value, axis, [(i, i ^ offset) for i in range(size)])


def after(value, dependency):
    if dependency is None:
        return value
    return lax.optimization_barrier((value, dependency))[0]


def contract_last(left, right):
    return lax.dot_general(left, right, (((1,), (1,)), ((), ())), preferred_element_type=F32)


def local_grads(gate, upper, hidden_grad):
    logistic = jax.nn.sigmoid(gate)
    gate_grad = hidden_grad * upper * logistic * (1.0 + gate * (1.0 - logistic))
    up_grad = hidden_grad * gate * logistic
    return jnp.stack([gate_grad.astype(BF16), up_grad.astype(BF16)])


def halves_swapped(value, flag, axis):
    first, second = jnp.split(value, 2, axis=axis)
    return jnp.concatenate(
        [jnp.where(flag, second, first), jnp.where(flag, first, second)], axis=axis
    )


def order_of(count):
    order = ["P0", "K0", "G0"]
    for n in range(1, count):
        order += [f"P{n}"]
        order += [f"G{n - 1}"] * (1 < n < count - 1)
        order += [f"K{n}"]
        order += [f"W{n - 2}"] * (2 < n < count - 1)
    if count > 2:
        order += [f"G{count - 2}"]
    left = [f"W{n}" for n in range(1, count) if f"W{n}" not in order] + ["W0"]
    last = f"G{count - 1}"
    if count == 1:
        return order + left
    return order + left[:1] + [last] + left[1:]


def solution(mesh):
    nx, ny, nz = mesh.shape["gx"], mesh.shape["gy"], mesh.shape["gz"]
    far = ny // 2

    def layer(inputs, out_grad, gate_weight, up_weight, down_weight):
        where_y = lax.axis_index("gy")
        odd, high = lax.rem(where_y, 2) == 1, where_y >= far
        rows = inputs.shape[0]
        half = rows // 2
        own = halves_swapped(jnp.stack([inputs, out_grad]), high, 1)

        columns = [own]
        for k in range(1, nz):
            low = k & -k
            if low == k:
                columns.append(swap(own, "gz", nz, k))
            else:
                columns.append(swap(columns[k - low], "gz", nz, low))

        pairs = [(k, i) for k in range(nz) for i in range(0, nx, 2)]
        count = len(pairs)
        partner_rows, core_sums, sent_far, grads_of = {}, {}, {}, {}
        totals = [None] * nz

        def fetch(n):
            k, i = pairs[n]
            even_block = swap(columns[k], "gx", nx, i)
            odd_block = swap(columns[k], "gx", nx, i + 1)
            return even_block, odd_block

        def project(n, token):
            even_block, odd_block = after(blocks[n], token)
            chunk = jnp.concatenate(
                [
                    jnp.where(odd, odd_block, even_block),
                    jnp.where(odd, even_block, odd_block),
                ],
                axis=1,
            )
            gate = jnp.dot(chunk[0], gate_weight, preferred_element_type=F32)
            upper = jnp.dot(chunk[0], up_weight, preferred_element_type=F32)
            hidden = contract_last(chunk[1], down_weight)
            terms = (gate, upper, hidden)
            sent = jnp.stack([t[rows:].astype(BF16) for t in terms])
            partner_rows[n] = swap(sent, "gy", ny, 1)
            core_sums[n] = [t[:rows] for t in terms]
            return sent

        def combine(n, token):
            got = after(partner_rows[n], token)
            terms = [t + g.astype(F32) for t, g in zip(core_sums[n], got)]
            sent = jnp.stack([t[half:].astype(BF16) for t in terms])
            sent_far[n] = swap(sent, "gy", ny, far)
            core_sums[n] = [t[:half] for t in terms]
            return sent

        def differentiate(n, token):
            got = after(sent_far[n], token)
            grads = local_grads(*[t + g.astype(F32) for t, g in zip(core_sums[n], got)])
            both = jnp.concatenate([grads, swap(grads, "gy", ny, far)], axis=1)
            grads_of[n] = (both, swap(both, "gy", ny, 1))
            return grads

        def backproject(n, token):
            k, i = pairs[n]
            grads = jnp.concatenate(after(grads_of[n], token), axis=1)
            partial = contract_last(grads[0], gate_weight) + contract_last(grads[1], up_weight)
            even_part = jnp.where(odd, partial[rows:], partial[:rows])
            odd_part = jnp.where(odd, partial[:rows], partial[rows:])
            for offset, part in ((i, even_part), (i + 1, odd_part)):
                if offset:
                    part = swap(part.astype(BF16), "gx", nx, offset).astype(F32)
                totals[k] = part if totals[k] is None else totals[k] + part
            return partial

        blocks = [fetch(n) for n in range(count)]
        token = None
        for stage in order_of(count):
            step = {"P": project, "K": combine, "G": differentiate, "W": backproject}[stage[0]]
            token = step(int(stage[1:]), token)
        received = totals[0]
        for k in range(1, nz):
            received = received + swap(totals[k].astype(BF16), "gz", nz, k).astype(F32)
        return halves_swapped(received, high, 0).astype(BF16)

    return jax.shard_map(
        layer,
        mesh=mesh,
        in_specs=(
            P(("gx", "gz"), "gy"),
            P(("gx", "gz"), "gy"),
            P("gy", ("gx", "gz")),
            P("gy", ("gx", "gz")),
            P(("gx", "gz"), "gy"),
        ),
        out_specs=P(("gx", "gz"), "gy"),
        check_vma=False,
    )
```
